256 devices in a mesh: row: 32 (over x_hi, z, core), ga: 8 (over x_lo, y).
Axes of the slice: x: 4 (x_hi: 2, x_lo: 2; x = x_hi * 2 + x_lo), y: 4, z: 8, core: 2. Of those that a mesh axis runs over, the one named last changes fastest.
Arguments:
- pair_dens: bfloat16 [32, 256, 4096], P('row', None, 'ga'), may hold values from -0.41992188 to 0.41992188
- cond_dens: bfloat16 [32, 1024, 4096], P('row', None, 'ga'), may hold values from -0.41992188 to 0.41992188
- val_dens: bfloat16 [32, 64, 4096], P(None, None, 'row'), may hold values from -0.41992188 to 0.41992188
- screened: bfloat16 [8, 4096, 4096], P(None, 'ga', 'row'), may hold values from -1 to 6, as said below
- coulomb: bfloat16 [4096], P('ga'), may hold values from 0.29882812 to 10
- pair_list: int32 [32, 256], replicated, may hold values from 0 to 255, each once within a row
- counts: int32 [32], replicated, may hold values from 10 to 256
- q_index: int32 [32], replicated, may hold values from 0 to 7
- column_k: int32 [1], replicated, may hold values from 0 to 31
Outputs:
- kernel: bfloat16 [8192, 256], P('row', 'ga')
The draws below stay inside these ranges and needn't reach their ends.
Inputs may be any that keep to these rules, and one draw needn't show every extreme that they name: `screened`: each diagonal entry exceeds the sum of the magnitudes of the others in its row divided by the square root of 4096 times four.
All inputs are finite; a program needn't handle non-finite values.
Results may differ from the reference program's by a relative error of at most 0.0042.
Values may be sent and summed in bfloat16 or wider, within the bound.
No kernel may reach another device: no remote copies, remote signals or barrier semaphores. Data moves between devices by JAX's collectives and lax.ppermute only.
A program may use at most 64 MiB of HBM per device.

```python
import math
import jax
import jax.numpy as jnp
from jax import lax

NV = 8
NC = 32
G = 4096
NQ = 8
PMAX = 256
VV = 64
NK = 32


def draw_screened(key, part):
    first = jax.random.fold_in(key, 11)
    second = jax.random.fold_in(key, 12)
    noise = jnp.clip(jax.random.normal(first, (NQ, G, G)), -4.0, 4.0)
    diag = jnp.exp(jax.random.uniform(second, (NQ, G), minval=0.0, maxval=math.log(5.0)))
    same = jnp.arange(G)[:, None] == jnp.arange(G)[None, :]
    return (noise / math.sqrt(G) + jnp.where(same[None, :, :], diag[:, :, None], 0.0)).astype(jnp.bfloat16)


def place_ends(result, own_key, smallest, top_value):
    dims = result.shape
    index_at = [jax.random.randint(jax.random.fold_in(own_key, axis), (), 0, dims[axis]) for axis in range(len(dims))]
    result = result.at[tuple(index_at)].set(smallest)
    longest = dims.index(max(dims))
    index_at[longest] = (index_at[longest] + 1) % dims[longest]
    return result.at[tuple(index_at)].set(top_value)


def shard_levels(stream_key, shape, shards, low, largest):
    def one(dim, shards_of):
        draws = jax.random.uniform(jax.random.fold_in(jax.random.fold_in(stream_key, 6), dim), (shards_of,), jnp.float32, low / len(shards), largest / len(shards))
        return jnp.repeat(jnp.exp(draws), shape[dim] // shards_of).reshape((-1,) + (1,) * (len(shape) - dim - 1))

    loudness = one(*shards[0])
    for cut in shards[1:]:
        loudness = loudness * one(*cut)
    return loudness


def gaussian(rng, extent, width, limit, pieces=(), kind=jnp.bfloat16):
    result = width * jax.random.normal(rng, extent, jnp.float32)
    if pieces:
        result = result * shard_levels(rng, extent, pieces, -0.22, 0.18)
    return jnp.clip(result, -limit, limit).astype(kind)


def setup_inputs(seed: int = 0) -> dict:
    keys = jax.random.split(jax.random.key(seed), 10)
    pair_dens = gaussian(keys[0], (NK, PMAX, G), 0.07, 0.41992188, ((0, 32), (2, 8)))
    cond_dens = gaussian(keys[1], (NK, NC * NC, G), 0.07, 0.41992188, ((0, 32), (2, 8)))
    val_dens = gaussian(keys[2], (NK, VV, G), 0.07, 0.41992188, ((2, 32),))
    screened = draw_screened(jax.random.fold_in(keys[9], 71), 0)
    coulomb = jnp.clip(jnp.exp(math.log(10.0) - 3.5104718 * jax.random.uniform(keys[4], (G,), jnp.float32) ** shard_levels(keys[4], (G,), ((0, 8),), -0.2, 0.2)), 0.29882812, 10.0).astype(jnp.bfloat16)
    pair_list = jax.vmap(lambda own: jax.random.permutation(own, PMAX))(jax.random.split(keys[5], NK)).reshape((NK, PMAX)).astype(jnp.int32)
    counts = place_ends(jax.random.randint(keys[6], (NK,), max(2, NV * NC // 25), min(401, NV * NC + 1)), jax.random.fold_in(keys[6], 1), max(2, NV * NC // 25), (min(401, NV * NC + 1)) - 1).astype(jnp.int32)
    q_index = place_ends(jax.random.randint(keys[7], (NK,), 0, NQ), jax.random.fold_in(keys[7], 1), 0, NQ - 1).astype(jnp.int32)
    column_k = jax.random.randint(keys[8], (1,), 0, NK).astype(jnp.int32)
    return {"pair_dens": pair_dens, "cond_dens": cond_dens, "val_dens": val_dens, "screened": screened, "coulomb": coulomb, "pair_list": pair_list, "counts": counts, "q_index": q_index, "column_k": column_k}


def reference(pair_dens, cond_dens, val_dens, screened, coulomb, pair_list, counts, q_index, column_k):
    column = column_k[0]
    col_pairs = pair_list[column]
    col = jnp.take(pair_dens[column], col_pairs, axis=0)
    col_count = counts[column]
    slots = jnp.arange(NV * NC, dtype=jnp.int32)
    col_mask = (slots < col_count).astype(jnp.float32)

    def one_point(index):
        pairs = pair_list[index]
        rows = jnp.take(pair_dens[index], pairs, axis=0)
        weighted = (rows.astype(jnp.float32) * coulomb.astype(jnp.float32)[None, :]).astype(jnp.bfloat16)
        exch = jnp.dot(weighted, col.T, preferred_element_type=jnp.float32)
        wmat = screened[q_index[index]]
        screened_val = jnp.dot(val_dens[index], wmat.T, preferred_element_type=jnp.float32).astype(jnp.bfloat16)
        direct_full = jnp.dot(cond_dens[index], screened_val.T, preferred_element_type=jnp.float32)
        arranged = direct_full.reshape(NC, NC, NV, NV).transpose(2, 0, 3, 1).reshape(NV * NC, NV * NC)
        direct = jnp.take(jnp.take(arranged, pairs, axis=0), col_pairs, axis=1)
        row_mask = (slots < counts[index]).astype(jnp.float32)
        block = (2.0 * exch - direct) * row_mask[:, None] * col_mask[None, :]
        return block.astype(jnp.bfloat16)

    blocks = lax.map(one_point, jnp.arange(pair_dens.shape[0], dtype=jnp.int32))
    return blocks.reshape(pair_dens.shape[0] * NV * NC, NV * NC)
```

```python
import jax
import jax.numpy as jnp
from jax import lax
from jax.experimental import pallas as pl
from jax.experimental.pallas import tpu as pltpu
from jax.sharding import Mesh
from jax.sharding import PartitionSpec as P

NV = 8
NC = 32
XH, Z, CORE, XL, Y = 2, 8, 2, 2, 4
ROW = ("xh", "z", "core")
GA = ("xl", "y")
BF = jnp.bfloat16
F32 = jnp.float32
VMEM = pl.BlockSpec(memory_space=pltpu.VMEM)
SMEM = pl.BlockSpec(memory_space=pltpu.SMEM)
LAST = (((1,), (1,)), ((), ()))


def call(body, out, specs, flops=1 << 20, nbytes=1 << 20):
    many = isinstance(out, (list, tuple))
    return pl.pallas_call(
        body,
        out_shape=out,
        in_specs=specs,
        out_specs=tuple(VMEM for _ in out) if many else VMEM,
        cost_estimate=pl.CostEstimate(flops=flops, bytes_accessed=nbytes, transcendentals=0),
    )


def shaped(shape, dtype):
    return jax.ShapeDtypeStruct(shape, dtype)


def dot(a, b):
    return lax.dot_general(a, b, LAST, preferred_element_type=F32)


def partial_sums(other_x, other_core, q_index, val, screened, added, dtype):
    planes, vv, hh = Z, val.shape[1], screened.shape[1]

    def body(q_ref, val_ref, w_ref, *refs):
        out_ref = refs[-1]
        xh, core = lax.axis_index("xh"), lax.axis_index("core")
        xh = 1 - xh if other_x else xh
        core = 1 - core if other_core else core
        for z in range(planes):
            k = (xh * Z + z) * CORE + core
            r = dot(val_ref[k], w_ref[q_ref[k]])
            if len(refs) == 2:
                r = r + refs[0][z].astype(F32)
            out_ref[z] = r.astype(dtype)

    args = (q_index, val, screened) + (() if added is None else (added,))
    specs = [SMEM, VMEM, VMEM] + ([] if added is None else [VMEM])
    flops = 2 * planes * vv * hh * val.shape[2]
    return call(body, shaped((planes, vv, hh), dtype), specs, flops, 2 << 20)(*args)


def half_of_column(column, own, sib):
    half = own.shape[1] // 2

    def body(c_ref, own_ref, sib_ref, out_ref):
        core = lax.axis_index("core")
        rows = pl.ds(pl.multiple_of(core * half, half), half)
        mine = c_ref[0] % CORE == core

        @pl.when(mine)
        def _():
            out_ref[...] = own_ref[0, rows, :]

        @pl.when(jnp.logical_not(mine))
        def _():
            out_ref[...] = sib_ref[0, rows, :]

    return call(body, shaped((half, own.shape[2]), BF), [SMEM, VMEM, VMEM])(column, own, sib)


def piece_for_all(column, parts):
    def body(c_ref, in_ref, out_ref):
        z = (c_ref[0] // CORE) % Z
        piece = in_ref[z]
        for i in range(Z):
            out_ref[i] = piece

    return call(body, shaped(parts.shape, BF), [SMEM, VMEM])(column, parts)


def exchange_terms(column, counts, pair_list, pair_dens, coulomb, halves):
    slots, g = pair_dens.shape[1:]
    half = slots // 2

    def body(c_ref, n_ref, pl_ref, pd_ref, cou_ref, own_ref, sib_ref, ox_ref, sx_ref, ex_ref, pt_ref, ps_ref, col_ref):
        xh, z, core = (lax.axis_index(a) for a in ROW)
        k = (xh * Z + z) * CORE + core
        ck = c_ref[0]
        same = ck // (Z * CORE) == xh
        first = pl.ds(pl.multiple_of(core * half, half), half)
        second = pl.ds(pl.multiple_of((1 - core) * half, half), half)

        @pl.when(same)
        def _():
            col_ref[first, :] = own_ref[...]
            col_ref[second, :] = sib_ref[...]

        @pl.when(jnp.logical_not(same))
        def _():
            col_ref[first, :] = ox_ref[...]
            col_ref[second, :] = sx_ref[...]

        weighted = (pd_ref[0].astype(F32) * cou_ref[...].astype(F32)).astype(BF)
        ex_ref[...] = 2.0 * dot(col_ref[...], weighted)
        pair = lax.broadcasted_iota(jnp.int32, (slots, slots), 0)
        slot = lax.broadcasted_iota(jnp.int32, (slots, slots), 1)
        mine = (pair == pl_ref[pl.ds(k, 1), :]) & (slot < n_ref[k])
        ps_ref[...] = mine.astype(F32).astype(BF)
        theirs = (pair == pl_ref[pl.ds(ck, 1), :]) & (slot < n_ref[ck])
        pt_ref[...] = theirs.astype(F32).T.astype(BF)

    square = (slots, slots)
    return pl.pallas_call(
        body,
        out_shape=(shaped(square, F32), shaped(square, BF), shaped(square, BF)),
        in_specs=[SMEM, SMEM] + [VMEM] * 7,
        out_specs=(VMEM, VMEM, VMEM),
        scratch_shapes=[pltpu.VMEM((slots, g), BF)],
        cost_estimate=pl.CostEstimate(flops=2 * slots * slots * g, bytes_accessed=1 << 20, transcendentals=0),
    )(column, counts, pair_list, pair_dens, coulomb.reshape(1, g), *halves)


def combine(arrived, cond_t, ex2, pt):
    slots = ex2.shape[0]
    vv, hh = arrived.shape[1:]

    def body(y_ref, cond_ref, ex_ref, pt_ref, out_ref, s_ref):
        sv = jnp.sum(y_ref[...].astype(F32), axis=0).astype(BF)
        r = dot(sv, cond_ref[...])
        for c in range(NC):
            s_ref[pl.ds(c, vv, stride=NC), :] = r[:, c * NC : (c + 1) * NC]
        direct = jnp.concatenate([s_ref[v * slots : (v + 1) * slots, :] for v in range(NV)], axis=1)
        terms = (ex_ref[...] - direct).astype(BF)
        out_ref[...] = jnp.dot(pt_ref[...], terms, preferred_element_type=F32).astype(BF)

    return pl.pallas_call(
        body,
        out_shape=shaped((slots, slots), BF),
        in_specs=[VMEM] * 4,
        out_specs=VMEM,
        scratch_shapes=[pltpu.VMEM((vv * NC, NC), F32)],
        cost_estimate=pl.CostEstimate(flops=2 * vv * NC * NC * hh, bytes_accessed=2 << 20, transcendentals=0),
    )(arrived, cond_t, ex2, pt)


def finish(parts, ps):
    def body(in_ref, ps_ref, out_ref):
        total = jnp.sum(in_ref[...].astype(F32), axis=0).astype(BF)
        out_ref[...] = jnp.dot(total, ps_ref[...], preferred_element_type=F32).astype(BF)

    return call(body, shaped(parts.shape[1:], BF), [VMEM, VMEM])(parts, ps)


def swap(x, axis):
    return lax.ppermute(x, axis, [(0, 1), (1, 0)])


def per_device(
    pair_dens, cond_dens, val_dens, screened, coulomb, pair_list, counts, q_index, column_k
):
    slots, g = pair_dens.shape[1:]
    terms = lambda ox, oc, added, dtype: partial_sums(ox, oc, q_index, val_dens, screened, added, dtype)
    to_core = swap(terms(True, True, None, BF), "core")
    sib = swap(pair_dens, "core")
    to_x = terms(True, False, to_core, BF)
    from_x = swap(to_x, "xh")
    to_core_2 = swap(terms(False, True, None, BF), "core")
    own = terms(False, False, to_core_2, F32)
    half = half_of_column(column_k, pair_dens, sib)
    parts = lax.all_to_all(half.reshape(Z, -1, g), "z", 0, 0, tiled=True)
    spread = lax.all_to_all(piece_for_all(column_k, parts), "z", 0, 0, tiled=True)
    own_half = spread.reshape(half.shape)
    sib_half = swap(own_half, "core")
    own_half_x = swap(own_half, "xh")
    sib_half_x = swap(sib_half, "xh")
    to_z = (own + from_x.astype(F32)).astype(BF)
    arrived = lax.all_to_all(to_z, "z", 0, 0, tiled=True)
    ex2, pt, ps = exchange_terms(
        column_k, counts, pair_list, pair_dens, coulomb, (own_half, sib_half, own_half_x, sib_half_x)
    )
    cond_t = cond_dens.reshape(NC, NC, g).transpose(1, 0, 2).reshape(NC * NC, g)
    combined = combine(arrived, cond_t, ex2, pt)
    blocks = lax.all_to_all(combined.reshape(XL * Y, -1, slots), GA, 0, 0, tiled=True)
    return finish(blocks, ps).T


def solution(mesh):
    fine = Mesh(mesh.devices.reshape(XH, Z, CORE, XL, Y), ROW + GA)
    placed = (
        P(ROW, None, GA),
        P(ROW, None, GA),
        P(None, None, ROW),
        P(None, GA, ROW),
        P(GA),
        P(),
        P(),
        P(),
        P(),
    )
    return jax.shard_map(
        per_device, mesh=fine, in_specs=placed, out_specs=P(ROW, GA), check_vma=False
    )
```

```python
import jax
import jax.numpy as jnp
from jax import lax
from jax.experimental import pallas as pl
from jax.experimental.pallas import tpu as pltpu
from jax.sharding import Mesh
from jax.sharding import PartitionSpec as P


NV = 8
NC = 32
XH, Z, CORE, XL, Y = 2, 8, 2, 2, 4
ROW = ("xh", "z", "core")
GA = ("xl", "y")
BF = jnp.bfloat16
F32 = jnp.float32
VMEM = pl.BlockSpec(memory_space=pltpu.VMEM)
SMEM = pl.BlockSpec(memory_space=pltpu.SMEM)
ANY = pl.BlockSpec(memory_space=pl.ANY)
LAST = (((1,), (1,)), ((), ()))


def near(x):
    return pltpu.with_memory_space_constraint(x, pltpu.VMEM)


def call(body, out, scalars, arrays, after=(), scratch=(), limit=12 << 20, flops=1 << 20, nbytes=1 << 20):
    many = isinstance(out, (list, tuple))
    n_in, n_after = len(scalars) + len(arrays), len(after)

    def run(*refs):
        body(*refs[:n_in], *refs[n_in + n_after :])

    return pl.pallas_call(
        run,
        out_shape=out,
        in_specs=[SMEM] * len(scalars) + [VMEM] * len(arrays) + [ANY] * n_after,
        out_specs=tuple(SMEM if o.memory_space == pltpu.SMEM else VMEM for o in out) if many else VMEM,
        scratch_shapes=list(scratch),
        compiler_params=pltpu.CompilerParams(vmem_limit_bytes=limit),
        cost_estimate=pl.CostEstimate(flops=flops, bytes_accessed=nbytes, transcendentals=0),
    )(*scalars, *arrays, *after)


def dot(a, b):
    return lax.dot_general(a, b, LAST, preferred_element_type=F32)


def partial_terms(refs, other_x, other_core, emit):
    q_ref, val_ref, w_ref = refs
    xh, core = lax.axis_index("xh"), lax.axis_index("core")
    xh = 1 - xh if other_x else xh
    core = 1 - core if other_core else core
    for z in range(Z):
        k = (xh * Z + z) * CORE + core
        emit(z, dot(val_ref[k], w_ref[q_ref[k]]))


def to_other_core(q_index, val, screened, after=()):
    def body(q_ref, val_ref, w_ref, out_ref):
        def emit(z, r):
            out_ref[z] = r.astype(BF)

        partial_terms((q_ref, val_ref, w_ref), False, True, emit)

    return call(body, pltpu.VMEM((Z, val.shape[1], screened.shape[1]), BF), [q_index], [val, screened], after)


def first_terms(q_index, val, screened):
    def body(q_ref, val_ref, w_ref, out_ref, val_out, w_out, q_out):
        def emit(z, r):
            out_ref[z] = r.astype(BF)

        for k in range(q_ref.shape[0]):
            q_out[k] = q_ref[k]

        partial_terms((q_ref, val_ref, w_ref), True, True, emit)
        val_out[...] = val_ref[...]
        w_out[...] = w_ref[...]

    out = (
        pltpu.VMEM((Z, val.shape[1], screened.shape[1]), BF),
        pltpu.VMEM(val.shape, BF),
        pltpu.VMEM(screened.shape, BF),
        pltpu.SMEM(q_index.shape, jnp.int32),
    )
    return call(body, out, [q_index], [val, screened], limit=64_400_000)


def to_other_x(q_index, val, screened, arrived, after=()):
    def body(q_ref, val_ref, w_ref, in_ref, out_ref):
        def emit(z, r):
            out_ref[z] = (r + in_ref[z].astype(F32)).astype(BF)

        partial_terms((q_ref, val_ref, w_ref), True, False, emit)

    return call(body, pltpu.VMEM(arrived.shape, BF), [q_index], [val, screened, arrived], after)


def own_terms(q_index, val, screened, arrived):
    def body(q_ref, val_ref, w_ref, in_ref, out_ref):
        def emit(z, r):
            out_ref[z] = r + in_ref[z].astype(F32)

        partial_terms((q_ref, val_ref, w_ref), False, False, emit)

    return call(body, pltpu.VMEM(arrived.shape, F32), [q_index], [val, screened, arrived])


def prepare(column, counts, pair_list, pair_dens, coulomb):
    slots, g = pair_dens.shape[1:]

    def body(c_ref, n_ref, pl_ref, pd_ref, cou_ref, weighted_ref, pt_ref, ps_ref):
        xh, z, core = (lax.axis_index(a) for a in ROW)
        k = (xh * Z + z) * CORE + core
        ck = c_ref[0]
        weighted_ref[...] = (pd_ref[0].astype(F32) * cou_ref[...].astype(F32)).astype(BF)
        pair = lax.broadcasted_iota(jnp.int32, (slots, slots), 0)
        slot = lax.broadcasted_iota(jnp.int32, (slots, slots), 1)
        mine = (pair == pl_ref[pl.ds(k, 1), :]) & (slot < n_ref[k])
        ps_ref[...] = mine.astype(F32).astype(BF)
        theirs = (pair == pl_ref[pl.ds(ck, 1), :]) & (slot < n_ref[ck])
        pt_ref[...] = theirs.astype(F32).T.astype(BF)

    out = (pltpu.VMEM((slots, g), BF), pltpu.VMEM((slots, slots), BF), pltpu.VMEM((slots, slots), BF))
    return call(body, out, [column, counts], [pair_list, pair_dens, coulomb.reshape(1, g)])


def half_of_column(column, own, sib):
    half = own.shape[1] // CORE

    def body(c_ref, own_ref, sib_ref, out_ref):
        core = lax.axis_index("core")
        rows = pl.ds(pl.multiple_of(core * half, half), half)
        mine = c_ref[0] % CORE == core

        @pl.when(mine)
        def _():
            out_ref[...] = own_ref[0, rows, :]

        @pl.when(jnp.logical_not(mine))
        def _():
            out_ref[...] = sib_ref[0, rows, :]

    return call(body, pltpu.VMEM((half, own.shape[2]), BF), [column], [own, sib])


def pick(column, own, below, above, reach, after=()):
    def body(c_ref, own_ref, below_ref, above_ref, out_ref):
        d = (lax.axis_index("z") - (c_ref[0] // CORE) % Z + Z) % Z
        low = (d > reach) & (d <= Z // 2) if reach else d == 1
        high = (d > Z // 2) & (d < Z - reach) if reach else d == Z - 1

        @pl.when(low)
        def _():
            out_ref[...] = below_ref[...]

        @pl.when(high)
        def _():
            out_ref[...] = above_ref[...]

        @pl.when(jnp.logical_not(low | high))
        def _():
            out_ref[...] = own_ref[...]

    return call(body, pltpu.VMEM(own.shape, BF), [column], [own, below, above], after)


def pick_x(column, own, other):
    def body(c_ref, own_ref, other_ref, out_ref):
        same = c_ref[0] // (Z * CORE) == lax.axis_index("xh")

        @pl.when(same)
        def _():
            out_ref[...] = own_ref[...]

        @pl.when(jnp.logical_not(same))
        def _():
            out_ref[...] = other_ref[...]

    return call(body, pltpu.VMEM(own.shape, BF), [column], [own, other])


def add(own, arrived):
    def body(own_ref, in_ref, out_ref):
        for z in range(Z):
            out_ref[z] = (own_ref[z] + in_ref[z].astype(F32)).astype(BF)

    return call(body, pltpu.VMEM(own.shape, BF), [], [own, arrived])


def exchange_terms(weighted, own_half, sib_half):
    slots = weighted.shape[0]
    half = slots // CORE

    def body(weighted_ref, own_ref, sib_ref, ex_ref):
        own = 2.0 * dot(weighted_ref[...], own_ref[...])
        sib = 2.0 * dot(weighted_ref[...], sib_ref[...])
        low = lax.axis_index("core") == 0
        ex_ref[:, :half] = jnp.where(low, own, sib)
        ex_ref[:, half:] = jnp.where(low, sib, own)

    return call(body, pltpu.VMEM((slots, slots), F32), [], [weighted, own_half, sib_half])


def combine(arrived, cond, ex2, pt):
    slots = ex2.shape[0]
    vv = arrived.shape[1]

    def body(y_ref, cond_ref, ex_ref, pt_ref, out_ref, s_ref):
        sv = jnp.sum(y_ref[...].astype(F32), axis=0).astype(BF)
        i = lax.broadcasted_iota(jnp.int32, (vv, vv), 0)
        j = lax.broadcasted_iota(jnp.int32, (vv, vv), 1)
        turn = (j == (i % NV) * NV + i // NV).astype(F32).astype(BF)
        sv = jnp.dot(turn, sv, preferred_element_type=F32).astype(BF)
        r = dot(sv, cond_ref[0])
        for c in range(NC):
            s_ref[pl.ds(c, vv, stride=NC), :] = r[:, c * NC : (c + 1) * NC]
        direct = jnp.concatenate([s_ref[v * slots : (v + 1) * slots, :] for v in range(NV)], axis=1)
        terms = (ex_ref[...] - direct).astype(BF)
        out_ref[...] = dot(pt_ref[...], terms).astype(BF)

    return call(
        body, pltpu.VMEM((slots, slots), BF), [], [arrived, cond, ex2, pt], (), [pltpu.VMEM((vv * NC, NC), F32)]
    )


def finish(parts, ps):
    def body(in_ref, ps_ref, out_ref):
        total = jnp.sum(in_ref[...].astype(F32), axis=0).astype(BF)
        out_ref[...] = jnp.dot(total, ps_ref[...], preferred_element_type=F32).astype(BF)

    return call(body, jax.ShapeDtypeStruct(parts.shape[1:], BF), [], [parts, ps])


def shift(x, axis, size, by):
    return lax.ppermute(x, axis, [(i, (i + by) % size) for i in range(size)])


def swap(x, axis):
    return shift(x, axis, 2, 1)


def per_device(
    pair_dens, cond_dens, val_dens, screened, coulomb, pair_list, counts, q_index, column_k
):
    slots = pair_dens.shape[1]
    sib = swap(pair_dens, "core")
    to_core, val_near, screened_near, q_index = first_terms(q_index, val_dens, screened)
    from_core = swap(to_core, "core")
    to_x = to_other_x(q_index, val_near, screened_near, near(from_core))
    from_x = swap(to_x, "xh")
    to_core = to_other_core(q_index, val_near, screened_near, (to_x,))
    from_core_2 = swap(to_core, "core")
    own = own_terms(q_index, val_near, screened_near, near(from_core_2))
    weighted, pt, ps = prepare(column_k, counts, pair_list, pair_dens, coulomb)
    half = half_of_column(column_k, near(pair_dens), near(sib))
    ups, downs = (shift(half, "z", Z, by) for by in (1, -1))
    once = pick(column_k, half, near(ups), near(downs), 0)
    ups, downs = (shift(once, "z", Z, by) for by in (3, -3))
    own_half = pick(column_k, once, near(ups), near(downs), 1)
    own_half = pick_x(column_k, own_half, near(swap(own_half, "xh")))
    sib_half = swap(own_half, "core")
    to_z = add(own, near(from_x))
    arrived = lax.all_to_all(to_z, "z", 0, 0, tiled=True)
    ex2 = exchange_terms(weighted, own_half, near(sib_half))
    combined = combine(near(arrived), near(cond_dens), ex2, pt)
    blocks = lax.all_to_all(combined.reshape(XL * Y, -1, slots), GA, 0, 0, tiled=True)
    return finish(near(blocks), ps).T


def solution(mesh):
    fine = Mesh(mesh.devices.reshape(XH, Z, CORE, XL, Y), ROW + GA)
    placed = (
        P(ROW, None, GA),
        P(ROW, None, GA),
        P(None, None, ROW),
        P(None, GA, ROW),
        P(GA),
        P(),
        P(),
        P(),
        P(),
    )

    return jax.shard_map(per_device, mesh=fine, in_specs=placed, out_specs=P(ROW, GA), check_vma=False)
```

```python
import jax
import jax.numpy as jnp
from jax import lax
from jax.experimental import pallas as pl
from jax.experimental.pallas import tpu as pltpu
from jax.sharding import Mesh
from jax.sharding import PartitionSpec as P


NV = 8
NC = 32
XH, Z, CORE, XL, Y = 2, 8, 2, 2, 4
ROW = ("xh", "z", "core")
GA = ("xl", "y")
BF = jnp.bfloat16
F32 = jnp.float32
VMEM = pl.BlockSpec(memory_space=pltpu.VMEM)
SMEM = pl.BlockSpec(memory_space=pltpu.SMEM)
ANY = pl.BlockSpec(memory_space=pl.ANY)
LAST = (((1,), (1,)), ((), ()))


def near(x):
    return pltpu.with_memory_space_constraint(x, pltpu.VMEM)


def call(body, out, scalars, arrays, after=(), scratch=(), limit=12 << 20, flops=1 << 20, nbytes=1 << 20):
    many = isinstance(out, (list, tuple))
    n_in, n_after = len(scalars) + len(arrays), len(after)

    def run(*refs):
        body(*refs[:n_in], *refs[n_in + n_after :])

    return pl.pallas_call(
        run,
        out_shape=out,
        in_specs=[SMEM] * len(scalars) + [VMEM] * len(arrays) + [ANY] * n_after,
        out_specs=tuple(SMEM if o.memory_space == pltpu.SMEM else VMEM for o in out) if many else VMEM,
        scratch_shapes=list(scratch),
        compiler_params=pltpu.CompilerParams(vmem_limit_bytes=limit),
        cost_estimate=pl.CostEstimate(flops=flops, bytes_accessed=nbytes, transcendentals=0),
    )(*scalars, *arrays, *after)


def dot(a, b):
    return lax.dot_general(a, b, LAST, preferred_element_type=F32)


def partial_terms(refs, other_x, other_core, emit, planes=range(Z)):
    q_ref, val_ref, w_ref = refs
    xh, core = lax.axis_index("xh"), lax.axis_index("core")
    xh = 1 - xh if other_x else xh
    core = 1 - core if other_core else core
    for z in planes:
        k = (xh * Z + z) * CORE + core
        emit(z, dot(val_ref[k], w_ref[q_ref[k]]))


def to_other_core(q_index, val, screened, after=()):
    def body(q_ref, val_ref, w_ref, out_ref):
        def emit(z, r):
            out_ref[z] = r.astype(BF)

        partial_terms((q_ref, val_ref, w_ref), False, True, emit)

    return call(body, pltpu.VMEM((Z, val.shape[1], screened.shape[1]), BF), [q_index], [val, screened], after)


def first_terms(q_index, val, screened):
    half = Z // 2

    def body(q_ref, val_ref, w_ref, low_ref, high_ref, val_out, w_out, q_out):
        def emit(z, r):
            (low_ref if z < half else high_ref)[z % half] = r.astype(BF)

        for k in range(q_ref.shape[0]):
            q_out[k] = q_ref[k]

        partial_terms((q_ref, val_ref, w_ref), True, True, emit)
        val_out[...] = val_ref[...]
        w_out[...] = w_ref[...]

    out = (
        pltpu.VMEM((half, val.shape[1], screened.shape[1]), BF),
        pltpu.VMEM((half, val.shape[1], screened.shape[1]), BF),
        pltpu.VMEM(val.shape, BF),
        pltpu.VMEM(screened.shape, BF),
        pltpu.SMEM(q_index.shape, jnp.int32),
    )
    return call(body, out, [q_index], [val, screened], limit=64_400_000)


def to_other_x(q_index, val, screened, arrived, part, after=()):
    half = arrived.shape[0]

    def body(q_ref, val_ref, w_ref, in_ref, out_ref):
        def emit(z, r):
            out_ref[z % half] = (r + in_ref[z % half].astype(F32)).astype(BF)

        partial_terms((q_ref, val_ref, w_ref), True, False, emit, range(part * half, (part + 1) * half))

    return call(body, pltpu.VMEM(arrived.shape, BF), [q_index], [val, screened, arrived], after)


def own_terms(q_index, val, screened, arrived):
    def body(q_ref, val_ref, w_ref, in_ref, out_ref):
        def emit(z, r):
            out_ref[z] = r + in_ref[z].astype(F32)

        partial_terms((q_ref, val_ref, w_ref), False, False, emit)

    return call(body, pltpu.VMEM(arrived.shape, F32), [q_index], [val, screened, arrived])


def prepare(column, counts, pair_list, pair_dens, coulomb):
    slots, g = pair_dens.shape[1:]

    def body(c_ref, n_ref, pl_ref, pd_ref, cou_ref, weighted_ref, pt_ref, ps_ref):
        xh, z, core = (lax.axis_index(a) for a in ROW)
        k = (xh * Z + z) * CORE + core
        ck = c_ref[0]
        weighted_ref[...] = (pd_ref[0].astype(F32) * cou_ref[...].astype(F32)).astype(BF)
        pair = lax.broadcasted_iota(jnp.int32, (slots, slots), 0)
        slot = lax.broadcasted_iota(jnp.int32, (slots, slots), 1)
        mine = (pair == pl_ref[pl.ds(k, 1), :]) & (slot < n_ref[k])
        ps_ref[...] = mine.astype(F32).astype(BF)
        theirs = (pair == pl_ref[pl.ds(ck, 1), :]) & (slot < n_ref[ck])
        pt_ref[...] = theirs.astype(F32).T.astype(BF)

    out = (pltpu.VMEM((slots, g), BF), pltpu.VMEM((slots, slots), BF), pltpu.VMEM((slots, slots), BF))
    return call(body, out, [column, counts], [pair_list, pair_dens, coulomb.reshape(1, g)])


def half_of_column(column, own, sib):
    half = own.shape[1] // CORE

    def body(c_ref, own_ref, sib_ref, out_ref):
        core = lax.axis_index("core")
        rows = pl.ds(pl.multiple_of(core * half, half), half)
        mine = c_ref[0] % CORE == core

        @pl.when(mine)
        def _():
            out_ref[...] = own_ref[0, rows, :]

        @pl.when(jnp.logical_not(mine))
        def _():
            out_ref[...] = sib_ref[0, rows, :]

    return call(body, pltpu.VMEM((half, own.shape[2]), BF), [column], [own, sib])


def pick(column, own, below, above, reach, after=()):
    def body(c_ref, own_ref, below_ref, above_ref, out_ref):
        d = (lax.axis_index("z") - (c_ref[0] // CORE) % Z + Z) % Z
        low = (d > reach) & (d <= Z // 2) if reach else d == 1
        high = (d > Z // 2) & (d < Z - reach) if reach else d == Z - 1

        @pl.when(low)
        def _():
            out_ref[...] = below_ref[...]

        @pl.when(high)
        def _():
            out_ref[...] = above_ref[...]

        @pl.when(jnp.logical_not(low | high))
        def _():
            out_ref[...] = own_ref[...]

    return call(body, pltpu.VMEM(own.shape, BF), [column], [own, below, above], after)


def add(own, low, high):
    half = low.shape[0]

    def body(own_ref, low_ref, high_ref, out_ref):
        for z in range(Z):
            arrived = (low_ref if z < half else high_ref)[z % half]
            out_ref[z] = (own_ref[z] + arrived.astype(F32)).astype(BF)

    return call(body, pltpu.VMEM(own.shape, BF), [], [own, low, high])


def exchange_terms(column, weighted, halves):
    slots, g = weighted.shape
    half = slots // CORE

    def body(c_ref, weighted_ref, own_ref, sib_ref, own_x_ref, sib_x_ref, ex_ref, col_ref):
        core = lax.axis_index("core")
        same = c_ref[0] // (Z * CORE) == lax.axis_index("xh")
        first = pl.ds(pl.multiple_of(core * half, half), half)
        second = pl.ds(pl.multiple_of((1 - core) * half, half), half)

        @pl.when(same)
        def _():
            col_ref[first, :] = own_ref[...]
            col_ref[second, :] = sib_ref[...]

        @pl.when(jnp.logical_not(same))
        def _():
            col_ref[first, :] = own_x_ref[...]
            col_ref[second, :] = sib_x_ref[...]

        ex_ref[...] = 2.0 * dot(weighted_ref[...], col_ref[...])

    return call(
        body, pltpu.VMEM((slots, slots), F32), [column], [weighted, *halves], (), [pltpu.VMEM((slots, g), BF)]
    )


def combine(arrived, cond, ex2, pt):
    slots = ex2.shape[0]
    vv = arrived.shape[1]

    def body(y_ref, cond_ref, ex_ref, pt_ref, out_ref, s_ref):
        sv = y_ref[0].astype(F32)
        for z in range(1, Z):
            sv = sv + y_ref[z].astype(F32)
        r = dot(sv.astype(BF), cond_ref[0])
        for c in range(NC):
            for v in range(NV):
                block = r[v * NV : (v + 1) * NV, c * NC : (c + 1) * NC]
                s_ref[pl.ds(v * NC + c, NV, stride=slots), :] = block
        direct = jnp.concatenate([s_ref[v * slots : (v + 1) * slots, :] for v in range(NV)], axis=1)
        terms = (ex_ref[...] - direct).astype(BF)
        out_ref[...] = dot(pt_ref[...], terms).astype(BF)

    return call(
        body, pltpu.VMEM((slots, slots), BF), [], [arrived, cond, ex2, pt], (), [pltpu.VMEM((vv * NC, NC), F32)]
    )


def finish(parts, ps):
    def body(in_ref, ps_ref, out_ref):
        total = jnp.sum(in_ref[...].astype(F32), axis=0).astype(BF)
        out_ref[...] = jnp.dot(total, ps_ref[...], preferred_element_type=F32).astype(BF)

    return call(body, jax.ShapeDtypeStruct(parts.shape[1:], BF), [], [parts, ps])


def shift(x, axis, size, by):
    return lax.ppermute(x, axis, [(i, (i + by) % size) for i in range(size)])


def swap(x, axis):
    return shift(x, axis, 2, 1)


def per_device(
    pair_dens, cond_dens, val_dens, screened, coulomb, pair_list, counts, q_index, column_k
):
    slots = pair_dens.shape[1]
    sib = swap(pair_dens, "core")
    low, high, val_near, screened_near, q_index = first_terms(q_index, val_dens, screened)
    low = swap(low, "core")
    high = swap(high, "core")
    low = low_terms = to_other_x(q_index, val_near, screened_near, near(low), 0)
    high = to_other_x(q_index, val_near, screened_near, near(high), 1, (low,))
    low = swap(low, "xh")
    high = swap(high, "xh")
    to_core = to_other_core(q_index, val_near, screened_near, (low_terms,))
    from_core_2 = swap(to_core, "core")
    own = own_terms(q_index, val_near, screened_near, near(from_core_2))
    weighted, pt, ps = prepare(column_k, counts, pair_list, pair_dens, coulomb)
    half = half_of_column(column_k, near(pair_dens), near(sib))
    ups, downs = (shift(half, "z", Z, by) for by in (1, -1))
    once = pick(column_k, half, near(ups), near(downs), 0)
    ups, downs = (shift(once, "z", Z, by) for by in (3, -3))
    own_half = pick(column_k, once, near(ups), near(downs), 1)
    own_x = swap(own_half, "xh")
    sib_x = lax.ppermute(own_half, ("xh", "core"), [(i, 3 - i) for i in range(4)])
    sib_half = swap(own_half, "core")
    to_z = add(own, near(low), near(high))
    arrived = lax.all_to_all(to_z, "z", 0, 0, tiled=True)
    halves = [near(a) for a in (own_half, sib_half, own_x, sib_x)]
    ex2 = exchange_terms(column_k, weighted, halves)
    combined = combine(near(arrived), near(cond_dens), ex2, pt)
    blocks = lax.all_to_all(combined.reshape(XL * Y, -1, slots), GA, 0, 0, tiled=True)
    return finish(near(blocks), ps).T


def solution(mesh):
    fine = Mesh(mesh.devices.reshape(XH, Z, CORE, XL, Y), ROW + GA)
    placed = (
        P(ROW, None, GA),
        P(ROW, None, GA),
        P(None, None, ROW),
        P(None, GA, ROW),
        P(GA),
        P(),
        P(),
        P(),
        P(),
    )

    return jax.shard_map(per_device, mesh=fine, in_specs=placed, out_specs=P(ROW, GA), check_vma=False)
```

```python
import jax
import jax.numpy as jnp
from jax import lax
from jax.experimental import pallas as pl
from jax.experimental.pallas import tpu as pltpu
from jax.sharding import Mesh
from jax.sharding import PartitionSpec as P


NV = 8
NC = 32
XH, Z, CORE, XL, Y = 2, 8, 2, 2, 4
ROW = ("xh", "z", "core")
GA = ("xl", "y")
BF = jnp.bfloat16
F32 = jnp.float32
VMEM = pl.BlockSpec(memory_space=pltpu.VMEM)
SMEM = pl.BlockSpec(memory_space=pltpu.SMEM)
ANY = pl.BlockSpec(memory_space=pl.ANY)
LAST = (((1,), (1,)), ((), ()))


def near(x):
    return pltpu.with_memory_space_constraint(x, pltpu.VMEM)


def call(body, out, scalars, arrays, after=(), scratch=(), limit=12 << 20, flops=1 << 20, nbytes=1 << 20):
    many = isinstance(out, (list, tuple))
    n_in, n_after = len(scalars) + len(arrays), len(after)

    def run(*refs):
        body(*refs[:n_in], *refs[n_in + n_after :])

    return pl.pallas_call(
        run,
        out_shape=out,
        in_specs=[SMEM] * len(scalars) + [VMEM] * len(arrays) + [ANY] * n_after,
        out_specs=tuple(SMEM if o.memory_space == pltpu.SMEM else VMEM for o in out) if many else VMEM,
        scratch_shapes=list(scratch),
        compiler_params=pltpu.CompilerParams(vmem_limit_bytes=limit),
        cost_estimate=pl.CostEstimate(flops=flops, bytes_accessed=nbytes, transcendentals=0),
    )(*scalars, *arrays, *after)


def dot(a, b):
    return lax.dot_general(a, b, LAST, preferred_element_type=F32)


def partial_terms(refs, other_x, other_core, emit, planes=range(Z)):
    q_ref, val_ref, w_ref = refs
    xh, core = lax.axis_index("xh"), lax.axis_index("core")
    xh = 1 - xh if other_x else xh
    core = 1 - core if other_core else core
    for z in planes:
        k = (xh * Z + z) * CORE + core
        emit(z, dot(val_ref[k], w_ref[q_ref[k]]))


def to_other_core(other_x, group, q_index, val, screened, after=()):
    def body(q_ref, val_ref, w_ref, out_ref):
        def emit(z, r):
            out_ref[z - group[0]] = r.astype(BF)

        partial_terms((q_ref, val_ref, w_ref), other_x, True, emit, group)

    out = pltpu.VMEM((len(group), val.shape[1], screened.shape[1]), BF)
    return call(body, out, [q_index], [val, screened], after)


def first_terms(group, q_index, val, screened):
    def body(q_ref, val_ref, w_ref, out_ref, val_out, w_out, q_out):
        def emit(z, r):
            out_ref[z - group[0]] = r.astype(BF)

        for k in range(q_ref.shape[0]):
            q_out[k] = q_ref[k]
        partial_terms((q_ref, val_ref, w_ref), True, True, emit, group)
        val_out[...] = val_ref[...]
        w_out[...] = w_ref[...]

    out = (
        pltpu.VMEM((len(group), val.shape[1], screened.shape[1]), BF),
        pltpu.VMEM(val.shape, BF),
        pltpu.VMEM(screened.shape, BF),
        pltpu.SMEM(q_index.shape, jnp.int32),
    )
    return call(body, out, [q_index], [val, screened], limit=64_400_000)


def to_other_x(q_index, val, screened, arrived, part, after=()):
    half = arrived.shape[0]

    def body(q_ref, val_ref, w_ref, in_ref, out_ref):
        def emit(z, r):
            out_ref[z % half] = (r + in_ref[z % half].astype(F32)).astype(BF)

        partial_terms((q_ref, val_ref, w_ref), True, False, emit, range(part * half, (part + 1) * half))

    return call(body, pltpu.VMEM(arrived.shape, BF), [q_index], [val, screened, arrived], after)


def own_terms(q_index, val, screened, arrived):
    def body(q_ref, val_ref, w_ref, in_ref, out_ref):
        def emit(z, r):
            out_ref[z] = r + in_ref[z].astype(F32)

        partial_terms((q_ref, val_ref, w_ref), False, False, emit)

    return call(body, pltpu.VMEM(arrived.shape, F32), [q_index], [val, screened, arrived])


def prepare(column, counts, pair_list, pair_dens, coulomb):
    slots, g = pair_dens.shape[1:]

    def body(c_ref, n_ref, pl_ref, pd_ref, cou_ref, weighted_ref, pt_ref, ps_ref):
        xh, z, core = (lax.axis_index(a) for a in ROW)
        k = (xh * Z + z) * CORE + core
        ck = c_ref[0]
        weighted_ref[...] = (pd_ref[0].astype(F32) * cou_ref[...].astype(F32)).astype(BF)
        pair = lax.broadcasted_iota(jnp.int32, (slots, slots), 0)
        slot = lax.broadcasted_iota(jnp.int32, (slots, slots), 1)
        mine = (pair == pl_ref[pl.ds(k, 1), :]) & (slot < n_ref[k])
        ps_ref[...] = mine.astype(F32).astype(BF)
        theirs = (pair == pl_ref[pl.ds(ck, 1), :]) & (slot < n_ref[ck])
        pt_ref[...] = theirs.astype(F32).T.astype(BF)

    out = (pltpu.VMEM((slots, g), BF), pltpu.VMEM((slots, slots), BF), pltpu.VMEM((slots, slots), BF))
    return call(body, out, [column, counts], [pair_list, pair_dens, coulomb.reshape(1, g)])


def half_of_column(column, own, sib):
    half = own.shape[1] // CORE

    def body(c_ref, own_ref, sib_ref, out_ref):
        core = lax.axis_index("core")
        rows = pl.ds(pl.multiple_of(core * half, half), half)
        mine = c_ref[0] % CORE == core

        @pl.when(mine)
        def _():
            out_ref[...] = own_ref[0, rows, :]

        @pl.when(jnp.logical_not(mine))
        def _():
            out_ref[...] = sib_ref[0, rows, :]

    return call(body, pltpu.VMEM((half, own.shape[2]), BF), [column], [own, sib])


def pick(column, own, below, above, low, high):
    def body(c_ref, own_ref, below_ref, above_ref, out_ref):
        d = (lax.axis_index("z") - (c_ref[0] // CORE) % Z + Z) % Z
        from_below = (d >= low[0]) & (d <= low[1])
        from_above = (d >= high[0]) & (d <= high[1])

        @pl.when(from_below)
        def _():
            out_ref[...] = below_ref[...]

        @pl.when(from_above)
        def _():
            out_ref[...] = above_ref[...]

        @pl.when(jnp.logical_not(from_below | from_above))
        def _():
            out_ref[...] = own_ref[...]

    return call(body, pltpu.VMEM(own.shape, BF), [column], [own, below, above])


def add(own, low, high):
    half = low.shape[0]

    def body(own_ref, low_ref, high_ref, out_ref):
        for z in range(Z):
            arrived = (low_ref if z < half else high_ref)[z % half]
            out_ref[z] = (own_ref[z] + arrived.astype(F32)).astype(BF)

    return call(body, pltpu.VMEM(own.shape, BF), [], [own, low, high])


def exchange_terms(column, weighted, halves):
    slots, g = weighted.shape
    half = slots // CORE

    def body(c_ref, weighted_ref, own_ref, sib_ref, own_x_ref, sib_x_ref, ex_ref, col_ref):
        core = lax.axis_index("core")
        same = c_ref[0] // (Z * CORE) == lax.axis_index("xh")
        first = pl.ds(pl.multiple_of(core * half, half), half)
        second = pl.ds(pl.multiple_of((1 - core) * half, half), half)

        @pl.when(same)
        def _():
            col_ref[first, :] = own_ref[...]
            col_ref[second, :] = sib_ref[...]

        @pl.when(jnp.logical_not(same))
        def _():
            col_ref[first, :] = own_x_ref[...]
            col_ref[second, :] = sib_x_ref[...]

        ex_ref[...] = 2.0 * dot(weighted_ref[...], col_ref[...])

    return call(
        body, pltpu.VMEM((slots, slots), F32), [column], [weighted, *halves], (), [pltpu.VMEM((slots, g), BF)]
    )


def combine(arrived, cond, ex2, pt):
    slots = ex2.shape[0]
    vv = arrived.shape[1]

    def body(y_ref, cond_ref, ex_ref, pt_ref, out_ref, s_ref):
        sv = y_ref[0].astype(F32)
        for z in range(1, Z):
            sv = sv + y_ref[z].astype(F32)
        r = dot(sv.astype(BF), cond_ref[0])
        for c in range(NC):
            for v in range(NV):
                block = r[v * NV : (v + 1) * NV, c * NC : (c + 1) * NC]
                s_ref[pl.ds(v * NC + c, NV, stride=slots), :] = block
        direct = jnp.concatenate([s_ref[v * slots : (v + 1) * slots, :] for v in range(NV)], axis=1)
        terms = (ex_ref[...] - direct).astype(BF)
        out_ref[...] = dot(pt_ref[...], terms).astype(BF)

    return call(
        body, pltpu.VMEM((slots, slots), BF), [], [arrived, cond, ex2, pt], (), [pltpu.VMEM((vv * NC, NC), F32)]
    )


def finish(parts, ps):
    def body(in_ref, ps_ref, out_ref):
        total = jnp.sum(in_ref[...].astype(F32), axis=0).astype(BF)
        out_ref[...] = jnp.dot(total, ps_ref[...], preferred_element_type=F32).astype(BF)

    return call(body, jax.ShapeDtypeStruct(parts.shape[1:], BF), [], [parts, ps])


def shift(x, axis, size, by):
    return lax.ppermute(x, axis, [(i, (i + by) % size) for i in range(size)])


def swap(x, axis):
    return shift(x, axis, 2, 1)


def per_device(
    pair_dens, cond_dens, val_dens, screened, coulomb, pair_list, counts, q_index, column_k
):
    slots = pair_dens.shape[1]
    sib = swap(pair_dens, "core")
    groups = range(Z // 2), range(Z // 2, Z)
    low, val_near, screened_near, q_index = first_terms(groups[0], q_index, val_dens, screened)
    high = to_other_core(True, groups[1], q_index, val_near, screened_near)
    low = swap(low, "core")
    high = swap(high, "core")
    low = to_other_x(q_index, val_near, screened_near, near(low), 0)
    high = high_terms = to_other_x(q_index, val_near, screened_near, near(high), 1, (low,))
    low = swap(low, "xh")
    high = swap(high, "xh")
    to_core = to_other_core(False, range(Z), q_index, val_near, screened_near, (high_terms,))
    from_core_2 = swap(to_core, "core")
    own = own_terms(q_index, val_near, screened_near, near(from_core_2))
    weighted, pt, ps = prepare(column_k, counts, pair_list, pair_dens, coulomb)
    half = half_of_column(column_k, near(pair_dens), near(sib))
    ups, downs = (shift(half, "z", Z, by) for by in (1, -1))
    once = pick(column_k, half, near(ups), near(downs), (1, 1), (Z - 1, Z - 1))
    ups, downs = (shift(once, "z", Z, by) for by in (3, -2))
    own_half = pick(column_k, once, near(ups), near(downs), (2, 4), (5, 6))
    own_x = swap(own_half, "xh")
    sib_x = lax.ppermute(own_half, ("xh", "core"), [(i, 3 - i) for i in range(4)])
    sib_half = swap(own_half, "core")
    to_z = add(own, near(low), near(high))
    arrived = lax.all_to_all(to_z, "z", 0, 0, tiled=True)
    halves = [near(a) for a in (own_half, sib_half, own_x, sib_x)]
    ex2 = exchange_terms(column_k, weighted, halves)
    combined = combine(near(arrived), near(cond_dens), ex2, pt)
    blocks = lax.all_to_all(combined.reshape(XL * Y, -1, slots), GA, 0, 0, tiled=True)
    return finish(near(blocks), ps).T


def solution(mesh):
    fine = Mesh(mesh.devices.reshape(XH, Z, CORE, XL, Y), ROW + GA)
    placed = (
        P(ROW, None, GA),
        P(ROW, None, GA),
        P(None, None, ROW),
        P(None, GA, ROW),
        P(GA),
        P(),
        P(),
        P(),
        P(),
    )

    return jax.shard_map(per_device, mesh=fine, in_specs=placed, out_specs=P(ROW, GA), check_vma=False)
```

```python
import jax
import jax.numpy as jnp
from jax import lax
from jax.experimental import pallas as pl
from jax.experimental.pallas import tpu as pltpu
from jax.sharding import Mesh
from jax.sharding import PartitionSpec as P


NV = 8
NC = 32
XH, Z, CORE, XL, Y = 2, 8, 2, 2, 4
ROW = ("xh", "z", "core")
GA = ("xl", "y")
BF = jnp.bfloat16
F32 = jnp.float32
VMEM = pl.BlockSpec(memory_space=pltpu.VMEM)
SMEM = pl.BlockSpec(memory_space=pltpu.SMEM)
ANY = pl.BlockSpec(memory_space=pl.ANY)
LAST = (((1,), (1,)), ((), ()))


def near(x):
    return pltpu.with_memory_space_constraint(x, pltpu.VMEM)


def call(body, out, scalars, arrays, after=(), scratch=(), limit=12 << 20, flops=1 << 20, nbytes=1 << 20):
    many = isinstance(out, (list, tuple))
    n_in, n_after = len(scalars) + len(arrays), len(after)

    def run(*refs):
        body(*refs[:n_in], *refs[n_in + n_after :])

    return pl.pallas_call(
        run,
        out_shape=out,
        in_specs=[SMEM] * len(scalars) + [VMEM] * len(arrays) + [ANY] * n_after,
        out_specs=tuple(SMEM if o.memory_space == pltpu.SMEM else VMEM for o in out) if many else VMEM,
        scratch_shapes=list(scratch),
        compiler_params=pltpu.CompilerParams(vmem_limit_bytes=limit),
        cost_estimate=pl.CostEstimate(flops=flops, bytes_accessed=nbytes, transcendentals=0),
    )(*scalars, *arrays, *after)


def dot(a, b):
    return lax.dot_general(a, b, LAST, preferred_element_type=F32)


def partial_terms(refs, other_x, other_core, emit, planes=range(Z)):
    q_ref, val_ref, w_ref = refs
    xh, core = lax.axis_index("xh"), lax.axis_index("core")
    xh = 1 - xh if other_x else xh
    core = 1 - core if other_core else core
    for z in planes:
        k = (xh * Z + z) * CORE + core
        emit(z, dot(val_ref[k], w_ref[q_ref[k]]))


def to_other_core(other_x, group, q_index, val, screened, after=()):
    def body(q_ref, val_ref, w_ref, out_ref):
        def emit(z, r):
            out_ref[z - group[0]] = r.astype(BF)

        partial_terms((q_ref, val_ref, w_ref), other_x, True, emit, group)

    out = pltpu.VMEM((len(group), val.shape[1], screened.shape[1]), BF)
    return call(body, out, [q_index], [val, screened], after)


def first_terms(group, q_index, val, screened):
    def body(q_ref, val_ref, w_ref, out_ref, val_out, w_out, q_out):
        def emit(z, r):
            out_ref[z - group[0]] = r.astype(BF)

        for k in range(q_ref.shape[0]):
            q_out[k] = q_ref[k]
        partial_terms((q_ref, val_ref, w_ref), True, True, emit, group)
        val_out[...] = val_ref[...]
        w_out[...] = w_ref[...]

    out = (
        pltpu.VMEM((len(group), val.shape[1], screened.shape[1]), BF),
        pltpu.VMEM(val.shape, BF),
        pltpu.VMEM(screened.shape, BF),
        pltpu.SMEM(q_index.shape, jnp.int32),
    )
    return call(body, out, [q_index], [val, screened], limit=64_400_000)


def to_other_x(q_index, val, screened, arrived, part, after=()):
    half = arrived.shape[0]

    def body(q_ref, val_ref, w_ref, in_ref, out_ref):
        def emit(z, r):
            out_ref[z % half] = (r + in_ref[z % half].astype(F32)).astype(BF)

        partial_terms((q_ref, val_ref, w_ref), True, False, emit, range(part * half, (part + 1) * half))

    return call(body, pltpu.VMEM(arrived.shape, BF), [q_index], [val, screened, arrived], after)


def own_terms(q_index, val, screened, arrived):
    def body(q_ref, val_ref, w_ref, in_ref, out_ref):
        def emit(z, r):
            out_ref[z] = r + in_ref[z].astype(F32)

        partial_terms((q_ref, val_ref, w_ref), False, False, emit)

    return call(body, pltpu.VMEM(arrived.shape, F32), [q_index], [val, screened, arrived])


def prepare(column, counts, pair_list, pair_dens, coulomb):
    slots, g = pair_dens.shape[1:]

    def body(c_ref, n_ref, pl_ref, pd_ref, cou_ref, weighted_ref, pt_ref, ps_ref):
        xh, z, core = (lax.axis_index(a) for a in ROW)
        k = (xh * Z + z) * CORE + core
        ck = c_ref[0]
        weighted_ref[...] = (pd_ref[0].astype(F32) * cou_ref[...].astype(F32)).astype(BF)
        pair = lax.broadcasted_iota(jnp.int32, (slots, slots), 0)
        slot = lax.broadcasted_iota(jnp.int32, (slots, slots), 1)
        mine = (pair == pl_ref[pl.ds(k, 1), :]) & (slot < n_ref[k])
        ps_ref[...] = mine.astype(F32).astype(BF)
        theirs = (pair == pl_ref[pl.ds(ck, 1), :]) & (slot < n_ref[ck])
        pt_ref[...] = theirs.astype(F32).T.astype(BF)

    out = (pltpu.VMEM((slots, g), BF), pltpu.VMEM((slots, slots), BF), pltpu.VMEM((slots, slots), BF))
    return call(body, out, [column, counts], [pair_list, pair_dens, coulomb.reshape(1, g)])


def half_of_column(column, own, sib):
    half = own.shape[1] // CORE

    def body(c_ref, own_ref, sib_ref, out_ref):
        core = lax.axis_index("core")
        rows = pl.ds(pl.multiple_of(core * half, half), half)
        mine = c_ref[0] % CORE == core

        @pl.when(mine)
        def _():
            out_ref[...] = own_ref[0, rows, :]

        @pl.when(jnp.logical_not(mine))
        def _():
            out_ref[...] = sib_ref[0, rows, :]

    return call(body, pltpu.VMEM((half, own.shape[2]), BF), [column], [own, sib])


def pick(column, own, below, above, low, high):
    def body(c_ref, own_ref, below_ref, above_ref, out_ref):
        d = (lax.axis_index("z") - (c_ref[0] // CORE) % Z + Z) % Z
        from_below = (d >= low[0]) & (d <= low[1])
        from_above = (d >= high[0]) & (d <= high[1])

        @pl.when(from_below)
        def _():
            out_ref[...] = below_ref[...]

        @pl.when(from_above)
        def _():
            out_ref[...] = above_ref[...]

        @pl.when(jnp.logical_not(from_below | from_above))
        def _():
            out_ref[...] = own_ref[...]

    return call(body, pltpu.VMEM(own.shape, BF), [column], [own, below, above])


def add(own, low, high):
    half = low.shape[0]

    def body(own_ref, low_ref, high_ref, out_ref):
        for z in range(Z):
            arrived = (low_ref if z < half else high_ref)[z % half]
            out_ref[z] = (own_ref[z] + arrived.astype(F32)).astype(BF)

    return call(body, pltpu.VMEM(own.shape, BF), [], [own, low, high])


def exchange_terms(column, weighted, halves):
    slots, g = weighted.shape
    half = slots // CORE

    def body(c_ref, weighted_ref, own_ref, sib_ref, own_x_ref, sib_x_ref, ex_ref, col_ref):
        core = lax.axis_index("core")
        same = c_ref[0] // (Z * CORE) == lax.axis_index("xh")
        first = pl.ds(pl.multiple_of(core * half, half), half)
        second = pl.ds(pl.multiple_of((1 - core) * half, half), half)

        @pl.when(same)
        def _():
            col_ref[first, :] = own_ref[...]
            col_ref[second, :] = sib_ref[...]

        @pl.when(jnp.logical_not(same))
        def _():
            col_ref[first, :] = own_x_ref[...]
            col_ref[second, :] = sib_x_ref[...]

        ex_ref[...] = 2.0 * dot(weighted_ref[...], col_ref[...])

    return call(
        body, pltpu.VMEM((slots, slots), F32), [column], [weighted, *halves], (), [pltpu.VMEM((slots, g), BF)]
    )


def combine(arrived, cond, ex2, pt):
    slots = ex2.shape[0]
    vv, hh = arrived.shape[1:]

    def body(y_ref, cond_ref, ex_ref, pt_ref, out_ref, sv_ref, direct_ref):
        sv = y_ref[0].astype(F32)
        for z in range(1, Z):
            sv = sv + y_ref[z].astype(F32)
        for t in range(hh // 128):
            sv_ref[t] = sv[:, t * 128 : (t + 1) * 128]
        turned = jnp.concatenate(
            [
                jnp.concatenate([sv_ref[t, pl.ds(i, NV, stride=NV), :] for i in range(NV)], axis=0)
                for t in range(hh // 128)
            ],
            axis=1,
        )
        r = dot(turned.astype(BF), cond_ref[0])
        for c in range(NC):
            for j in range(2):
                blocks = [r[i * NV : (i + 1) * NV, c * NC : (c + 1) * NC] for i in range(4 * j, 4 * j + 4)]
                direct_ref[j, pl.ds(c, NV, stride=NC), :] = jnp.concatenate(blocks, axis=1)
        direct = jnp.concatenate([direct_ref[0], direct_ref[1]], axis=1)
        out_ref[...] = dot(pt_ref[...], (ex_ref[...] - direct).astype(BF)).astype(BF)

    scratch = [pltpu.VMEM((hh // 128, vv, 128), F32), pltpu.VMEM((2, slots, 128), F32)]
    return call(body, pltpu.VMEM((slots, slots), BF), [], [arrived, cond, ex2, pt], (), scratch)


def finish(parts, ps):
    def body(in_ref, ps_ref, out_ref):
        total = jnp.sum(in_ref[...].astype(F32), axis=0).astype(BF)
        out_ref[...] = jnp.dot(total, ps_ref[...], preferred_element_type=F32).astype(BF)

    return call(body, jax.ShapeDtypeStruct(parts.shape[1:], BF), [], [parts, ps])


def shift(x, axis, size, by):
    return lax.ppermute(x, axis, [(i, (i + by) % size) for i in range(size)])


def swap(x, axis):
    return shift(x, axis, 2, 1)


def per_device(
    pair_dens, cond_dens, val_dens, screened, coulomb, pair_list, counts, q_index, column_k
):
    slots = pair_dens.shape[1]
    sib = swap(pair_dens, "core")
    groups = range(Z // 2), range(Z // 2, Z)
    low, val_near, screened_near, q_index = first_terms(groups[0], q_index, val_dens, screened)
    high = to_other_core(True, groups[1], q_index, val_near, screened_near)
    low = swap(low, "core")
    high = swap(high, "core")
    low = to_other_x(q_index, val_near, screened_near, near(low), 0)
    high = high_terms = to_other_x(q_index, val_near, screened_near, near(high), 1, (low,))
    low = swap(low, "xh")
    high = swap(high, "xh")
    to_core = to_other_core(False, range(Z), q_index, val_near, screened_near, (high_terms,))
    from_core_2 = swap(to_core, "core")
    own = own_terms(q_index, val_near, screened_near, near(from_core_2))
    weighted, pt, ps = prepare(column_k, counts, pair_list, pair_dens, coulomb)
    half = half_of_column(column_k, near(pair_dens), near(sib))
    ups, downs = (shift(half, "z", Z, by) for by in (1, -1))
    once = pick(column_k, half, near(ups), near(downs), (1, 1), (Z - 1, Z - 1))
    ups, downs = (shift(once, "z", Z, by) for by in (3, -2))
    own_half = pick(column_k, once, near(ups), near(downs), (2, 4), (5, 6))
    own_x = swap(own_half, "xh")
    sib_x = lax.ppermute(own_half, ("xh", "core"), [(i, 3 - i) for i in range(4)])
    sib_half = swap(own_half, "core")
    to_z = add(own, near(low), near(high))
    arrived = lax.all_to_all(to_z, "z", 0, 0, tiled=True)
    halves = [near(a) for a in (own_half, sib_half, own_x, sib_x)]
    ex2 = exchange_terms(column_k, weighted, halves)
    combined = combine(near(arrived), near(cond_dens), ex2, pt)
    blocks = lax.all_to_all(combined.reshape(XL * Y, -1, slots), GA, 0, 0, tiled=True)
    return finish(near(blocks), ps).T


def solution(mesh):
    fine = Mesh(mesh.devices.reshape(XH, Z, CORE, XL, Y), ROW + GA)
    placed = (
        P(ROW, None, GA),
        P(ROW, None, GA),
        P(None, None, ROW),
        P(None, GA, ROW),
        P(GA),
        P(),
        P(),
        P(),
        P(),
    )

    return jax.shard_map(per_device, mesh=fine, in_specs=placed, out_specs=P(ROW, GA), check_vma=False)
```

```python
import jax
import jax.numpy as jnp
from jax import lax
from jax.experimental import pallas as pl
from jax.experimental.pallas import tpu as pltpu
from jax.sharding import Mesh
from jax.sharding import PartitionSpec as P


NV = 8
NC = 32
XH, Z, CORE, XL, Y = 2, 8, 2, 2, 4
ROW = ("xh", "z", "core")
GA = ("xl", "y")
BF = jnp.bfloat16
F32 = jnp.float32
VMEM = pl.BlockSpec(memory_space=pltpu.VMEM)
SMEM = pl.BlockSpec(memory_space=pltpu.SMEM)
ANY = pl.BlockSpec(memory_space=pl.ANY)
LAST = (((1,), (1,)), ((), ()))


def near(x):
    return pltpu.with_memory_space_constraint(x, pltpu.VMEM)


def call(body, out, scalars, arrays, after=(), scratch=(), limit=12 << 20, flops=1 << 20, nbytes=1 << 20):
    many = isinstance(out, (list, tuple))
    n_in, n_after = len(scalars) + len(arrays), len(after)

    def run(*refs):
        body(*refs[:n_in], *refs[n_in + n_after :])

    return pl.pallas_call(
        run,
        out_shape=out,
        in_specs=[SMEM] * len(scalars) + [VMEM] * len(arrays) + [ANY] * n_after,
        out_specs=tuple(SMEM if o.memory_space == pltpu.SMEM else VMEM for o in out) if many else VMEM,
        scratch_shapes=list(scratch),
        compiler_params=pltpu.CompilerParams(vmem_limit_bytes=limit),
        cost_estimate=pl.CostEstimate(flops=flops, bytes_accessed=nbytes, transcendentals=0),
    )(*scalars, *arrays, *after)


def dot(a, b):
    return lax.dot_general(a, b, LAST, preferred_element_type=F32)


def partial_terms(refs, other_x, other_core, emit, planes=range(Z)):
    q_ref, val_ref, w_ref = refs
    xh, core = lax.axis_index("xh"), lax.axis_index("core")
    xh = 1 - xh if other_x else xh
    core = 1 - core if other_core else core
    for z in planes:
        k = (xh * Z + z) * CORE + core
        emit(z, dot(val_ref[k], w_ref[q_ref[k]]))


def to_other_core(other_x, group, q_index, val, screened, after=()):
    def body(q_ref, val_ref, w_ref, out_ref):
        def emit(z, r):
            out_ref[z - group[0]] = r.astype(BF)

        partial_terms((q_ref, val_ref, w_ref), other_x, True, emit, group)

    out = pltpu.VMEM((len(group), val.shape[1], screened.shape[1]), BF)
    return call(body, out, [q_index], [val, screened], after)


def first_terms(group, q_index, val, screened):
    def body(q_ref, val_ref, w_ref, out_ref, val_out, w_out, q_out):
        def emit(z, r):
            out_ref[z - group[0]] = r.astype(BF)

        for k in range(q_ref.shape[0]):
            q_out[k] = q_ref[k]
        partial_terms((q_ref, val_ref, w_ref), True, True, emit, group)
        val_out[...] = val_ref[...]
        w_out[...] = w_ref[...]

    out = (
        pltpu.VMEM((len(group), val.shape[1], screened.shape[1]), BF),
        pltpu.VMEM(val.shape, BF),
        pltpu.VMEM(screened.shape, BF),
        pltpu.SMEM(q_index.shape, jnp.int32),
    )
    return call(body, out, [q_index], [val, screened], limit=64_400_000)


def to_other_x(q_index, val, screened, arrived, part, after=()):
    half = arrived.shape[0]

    def body(q_ref, val_ref, w_ref, in_ref, out_ref):
        def emit(z, r):
            out_ref[z % half] = (r + in_ref[z % half].astype(F32)).astype(BF)

        partial_terms((q_ref, val_ref, w_ref), True, False, emit, range(part * half, (part + 1) * half))

    return call(body, pltpu.VMEM(arrived.shape, BF), [q_index], [val, screened, arrived], after)


def own_terms(q_index, val, screened, arrived):
    def body(q_ref, val_ref, w_ref, in_ref, out_ref):
        def emit(z, r):
            out_ref[z] = r + in_ref[z].astype(F32)

        partial_terms((q_ref, val_ref, w_ref), False, False, emit)

    return call(body, pltpu.VMEM(arrived.shape, F32), [q_index], [val, screened, arrived])


def prepare(column, counts, pair_list, pair_dens, coulomb):
    slots, g = pair_dens.shape[1:]

    def body(c_ref, n_ref, pl_ref, pd_ref, cou_ref, weighted_ref, pt_ref, ps_ref):
        xh, z, core = (lax.axis_index(a) for a in ROW)
        k = (xh * Z + z) * CORE + core
        ck = c_ref[0]
        weighted_ref[...] = (pd_ref[0].astype(F32) * cou_ref[...].astype(F32)).astype(BF)
        pair = lax.broadcasted_iota(jnp.int32, (slots, slots), 0)
        slot = lax.broadcasted_iota(jnp.int32, (slots, slots), 1)
        mine = (pair == pl_ref[pl.ds(k, 1), :]) & (slot < n_ref[k])
        ps_ref[...] = mine.astype(F32).astype(BF)
        theirs = (pair == pl_ref[pl.ds(ck, 1), :]) & (slot < n_ref[ck])
        pt_ref[...] = theirs.astype(F32).T.astype(BF)

    out = (pltpu.VMEM((slots, g), BF), pltpu.VMEM((slots, slots), BF), pltpu.VMEM((slots, slots), BF))
    return call(body, out, [column, counts], [pair_list, pair_dens, coulomb.reshape(1, g)])


def half_of_column(column, own, sib):
    half = own.shape[1] // CORE

    def body(c_ref, own_ref, sib_ref, out_ref):
        core = lax.axis_index("core")
        rows = pl.ds(pl.multiple_of(core * half, half), half)
        mine = c_ref[0] % CORE == core

        @pl.when(mine)
        def _():
            out_ref[...] = own_ref[0, rows, :]

        @pl.when(jnp.logical_not(mine))
        def _():
            out_ref[...] = sib_ref[0, rows, :]

    return call(body, pltpu.VMEM((half, own.shape[2]), BF), [column], [own, sib])


def pick(column, own, below, above, low, high):
    def body(c_ref, own_ref, below_ref, above_ref, out_ref):
        d = (lax.axis_index("z") - (c_ref[0] // CORE) % Z + Z) % Z
        from_below = (d >= low[0]) & (d <= low[1])
        from_above = (d >= high[0]) & (d <= high[1])

        @pl.when(from_below)
        def _():
            out_ref[...] = below_ref[...]

        @pl.when(from_above)
        def _():
            out_ref[...] = above_ref[...]

        @pl.when(jnp.logical_not(from_below | from_above))
        def _():
            out_ref[...] = own_ref[...]

    return call(body, pltpu.VMEM(own.shape, BF), [column], [own, below, above])


def add(own, arrived, part, begun=None):
    half = arrived.shape[0]

    def body(own_ref, in_ref, *refs):
        for z in range(half):
            refs[-1][z] = (own_ref[part * half + z] + in_ref[z].astype(F32)).astype(BF)

    more = () if begun is None else (begun,)
    return pl.pallas_call(
        body,
        out_shape=jax.ShapeDtypeStruct(own.shape, BF),
        in_specs=[VMEM, VMEM] + [ANY for _ in more],
        grid=(1,),
        out_specs=pl.BlockSpec((half,) + own.shape[1:], lambda i: (part, 0, 0)),
        input_output_aliases={2: 0} if more else {},
        compiler_params=pltpu.CompilerParams(vmem_limit_bytes=12 << 20),
        cost_estimate=pl.CostEstimate(flops=1 << 20, bytes_accessed=1 << 19, transcendentals=0),
    )(own, arrived, *more)


def exchange_terms(column, weighted, halves):
    slots, g = weighted.shape
    half = slots // CORE

    def body(c_ref, weighted_ref, own_ref, sib_ref, own_x_ref, sib_x_ref, ex_ref, col_ref):
        core = lax.axis_index("core")
        same = c_ref[0] // (Z * CORE) == lax.axis_index("xh")
        first = pl.ds(pl.multiple_of(core * half, half), half)
        second = pl.ds(pl.multiple_of((1 - core) * half, half), half)

        @pl.when(same)
        def _():
            col_ref[first, :] = own_ref[...]
            col_ref[second, :] = sib_ref[...]

        @pl.when(jnp.logical_not(same))
        def _():
            col_ref[first, :] = own_x_ref[...]
            col_ref[second, :] = sib_x_ref[...]

        ex_ref[...] = 2.0 * dot(weighted_ref[...], col_ref[...])

    return call(
        body, pltpu.VMEM((slots, slots), F32), [column], [weighted, *halves], (), [pltpu.VMEM((slots, g), BF)]
    )


def combine(arrived, cond, ex2, pt):
    slots = ex2.shape[0]
    vv, hh = arrived.shape[1:]

    def body(y_ref, cond_ref, ex_ref, pt_ref, out_ref, sv_ref, direct_ref):
        sv = y_ref[0].astype(F32)
        for z in range(1, Z):
            sv = sv + y_ref[z].astype(F32)
        for t in range(hh // 128):
            sv_ref[t] = sv[:, t * 128 : (t + 1) * 128]
        turned = jnp.concatenate(
            [
                jnp.concatenate([sv_ref[t, pl.ds(i, NV, stride=NV), :] for i in range(NV)], axis=0)
                for t in range(hh // 128)
            ],
            axis=1,
        )
        r = dot(turned.astype(BF), cond_ref[0])
        for c in range(NC):
            for j in range(2):
                blocks = [r[i * NV : (i + 1) * NV, c * NC : (c + 1) * NC] for i in range(4 * j, 4 * j + 4)]
                direct_ref[j, pl.ds(c, NV, stride=NC), :] = jnp.concatenate(blocks, axis=1)
        direct = jnp.concatenate([direct_ref[0], direct_ref[1]], axis=1)
        out_ref[...] = dot(pt_ref[...], (ex_ref[...] - direct).astype(BF)).astype(BF)

    scratch = [pltpu.VMEM((hh // 128, vv, 128), F32), pltpu.VMEM((2, slots, 128), F32)]
    return call(body, pltpu.VMEM((slots, slots), BF), [], [arrived, cond, ex2, pt], (), scratch)


def finish(parts, ps):
    def body(in_ref, ps_ref, out_ref):
        total = jnp.sum(in_ref[...].astype(F32), axis=0).astype(BF)
        out_ref[...] = jnp.dot(total, ps_ref[...], preferred_element_type=F32).astype(BF)

    return call(body, jax.ShapeDtypeStruct(parts.shape[1:], BF), [], [parts, ps])


def shift(x, axis, size, by):
    return lax.ppermute(x, axis, [(i, (i + by) % size) for i in range(size)])


def swap(x, axis):
    return shift(x, axis, 2, 1)


def per_device(
    pair_dens, cond_dens, val_dens, screened, coulomb, pair_list, counts, q_index, column_k
):
    slots = pair_dens.shape[1]
    sib = swap(pair_dens, "core")
    groups = range(Z // 2), range(Z // 2, Z)
    low, val_near, screened_near, q_index = first_terms(groups[0], q_index, val_dens, screened)
    high = to_other_core(True, groups[1], q_index, val_near, screened_near)
    low = swap(low, "core")
    high = swap(high, "core")
    low = to_other_x(q_index, val_near, screened_near, near(low), 0)
    high = high_terms = to_other_x(q_index, val_near, screened_near, near(high), 1, (low,))
    low = swap(low, "xh")
    high = swap(high, "xh")
    to_core = to_other_core(False, range(Z), q_index, val_near, screened_near, (high_terms,))
    from_core_2 = swap(to_core, "core")
    own = own_terms(q_index, val_near, screened_near, near(from_core_2))
    weighted, pt, ps = prepare(column_k, counts, pair_list, pair_dens, coulomb)
    half = half_of_column(column_k, near(pair_dens), near(sib))
    ups, downs = (shift(half, "z", Z, by) for by in (1, -1))
    once = pick(column_k, half, near(ups), near(downs), (1, 1), (Z - 1, Z - 1))
    ups, downs = (shift(once, "z", Z, by) for by in (3, -2))
    own_half = pick(column_k, once, near(ups), near(downs), (2, 4), (5, 6))
    own_x = swap(own_half, "xh")
    sib_x = lax.ppermute(own_half, ("xh", "core"), [(i, 3 - i) for i in range(4)])
    sib_half = swap(own_half, "core")
    begun = add(own, near(low), 0)
    to_z = add(own, near(high), 1, begun)
    arrived = lax.all_to_all(to_z, "z", 0, 0, tiled=True)
    halves = [near(a) for a in (own_half, sib_half, own_x, sib_x)]
    ex2 = exchange_terms(column_k, weighted, halves)
    combined = combine(near(arrived), near(cond_dens), ex2, pt)
    blocks = lax.all_to_all(combined.reshape(XL * Y, -1, slots), GA, 0, 0, tiled=True)
    return finish(near(blocks), ps).T


def solution(mesh):
    fine = Mesh(mesh.devices.reshape(XH, Z, CORE, XL, Y), ROW + GA)
    placed = (
        P(ROW, None, GA),
        P(ROW, None, GA),
        P(None, None, ROW),
        P(None, GA, ROW),
        P(GA),
        P(),
        P(),
        P(),
        P(),
    )

    return jax.shard_map(per_device, mesh=fine, in_specs=placed, out_specs=P(ROW, GA), check_vma=False)
```
